16 devices in a mesh: dp: 2 (over y, z), tp: 8 (over x, core).
Axes of the slice: x: 4, y: 2, z: 1, core: 2. Of those that a mesh axis runs over, the one named last changes fastest.
The devices are a block of a 4x4x8 slice.
Arguments:
- x: bfloat16 [8192, 2048], P(('dp', 'tp')), parts along dimension 0
- dy: bfloat16 [8192, 2048], P(('dp', 'tp')), parts along dimension 0
- gate: bfloat16 [8192, 8192], P('dp', 'tp'), parts along dimension 0
- up: bfloat16 [8192, 8192], P('dp', 'tp'), parts along dimension 0
- w_gate: bfloat16 [2048, 8192], P(None, 'tp')
- w_up: bfloat16 [2048, 8192], P(None, 'tp')
- w_down: bfloat16 [8192, 2048], P('tp')
Outputs:
- output 1: bfloat16 [8192, 2048], P(('dp', 'tp')), parts along dimension 0
- output 2: bfloat16 [4096, 8192], P('dp', 'tp'), parts along dimension 0
- output 3: bfloat16 [4096, 8192], P('dp', 'tp'), parts along dimension 0
- output 4: bfloat16 [16384, 2048], P(('dp', 'tp')), parts along dimension 0
There are 2 independent parts. The reference program is written for one: setup_inputs(seed, part) draws one part's arguments, and reference() takes and returns one part's arrays. A program takes and returns all parts, laid end to end along the dimension named above; an argument that names none is the same for every part.
All inputs are finite; a program needn't handle non-finite values.
Results may differ from the reference program's by a relative error of at most 0.012.
Values are sent between devices in bfloat16 or wider.
A program may use at most 768 MiB of HBM per device.

```python
import jax
import jax.numpy as jnp

ROWS = 4096
D = 2048
FF = 8192


def act(gate, up):
    return jax.nn.silu(gate) * up


def setup_inputs(seed: int = 0, part: int = 0) -> dict:
    kx, ky, ka, kb, kg, ku, kd = jax.random.split(jax.random.key(seed), 7)
    kx, ky, ka, kb = (jax.random.fold_in(k, part) for k in (kx, ky, ka, kb))
    drawn = {
        "x": jax.random.normal(kx, (ROWS, D), jnp.float32),
        "dy": jax.random.normal(ky, (ROWS, D), jnp.float32),
        "gate": jax.random.normal(ka, (ROWS, FF), jnp.float32),
        "up": jax.random.normal(kb, (ROWS, FF), jnp.float32),
        "w_gate": jax.random.normal(kg, (D, FF), jnp.float32) * D**-0.5,
        "w_up": jax.random.normal(ku, (D, FF), jnp.float32) * D**-0.5,
        "w_down": jax.random.normal(kd, (FF, D), jnp.float32) * FF**-0.5,
    }
    return {k: v.astype(jnp.bfloat16) for k, v in drawn.items()}


def reference(x, dy, gate, up, w_gate, w_up, w_down):
    hidden, back = jax.vjp(act, gate.astype(jnp.float32), up.astype(jnp.float32))
    d_hidden = jnp.dot(dy, w_down.T, preferred_element_type=jnp.float32)
    d_gate, d_up = (g.astype(jnp.bfloat16) for g in back(d_hidden))
    dx = jnp.dot(d_gate, w_gate.T, preferred_element_type=jnp.float32) + jnp.dot(d_up, w_up.T, preferred_element_type=jnp.float32)
    dw_gate = jnp.dot(x.T, d_gate, preferred_element_type=jnp.float32)
    dw_up = jnp.dot(x.T, d_up, preferred_element_type=jnp.float32)
    dw_down = jnp.dot(hidden.astype(jnp.bfloat16).T, dy, preferred_element_type=jnp.float32)
    return tuple(g.astype(jnp.bfloat16) for g in (dx, dw_gate, dw_up, dw_down))
```

```python
import functools

import jax
import jax.numpy as jnp
from jax import lax
from jax.experimental import pallas as pl
from jax.experimental.pallas import tpu as pltpu
from jax.sharding import PartitionSpec as P

MESH = pl.DeviceIdType.MESH
NT = (((1,), (1,)), ((), ()))
TN = (((0,), (0,)), ((), ()))
F32, BF16 = jnp.float32, jnp.bfloat16
OWN, RIGHT, LEFT, OPP = range(4)
CHIP_STEP = (0, 1, 3, 2)

POS_A, POS_B, NEG_B, NEG_A, FWD_POS, FWD_NEG, SIB = range(7)
X0 = 10
SUM_SIB = 20
U2_POS, U2_NEG, U1_POS, U1_NEG, U3_POS, U3_NEG = range(24, 30)
N_COPIES = 30


def dot(a, b, dims):
    return lax.dot_general(a, b, dims, preferred_element_type=F32)


def kernel(n, x, dy, gate, up, wg_in, wu_in, wd_in,
           dx, dwg, dwu, dwd, dyf, xf, dgs, dus, sibr, sumr,
           wd, wg, wu, accd, accg, accu, act, gb, ub, dgb, dub, hb, sibst, sumst, last,
           send, recv, lsem, ssem, wsem):
    rows, d = x.shape
    f = gate.shape[1]
    half = rows // 2
    me = lax.axis_index("tp")
    core = lax.rem(me, 2)
    chip = lax.div(me, 2)
    chips = n // 2
    right, left = lax.rem(me + 2, n), lax.rem(me + n - 2, n)
    sib = me + 1 - 2 * core

    def at(ref, start, size):
        if not isinstance(start, int):
            start = pl.multiple_of(start, size)
        return ref.at[pl.ds(start, size)]

    def slot(q, m, h=None):
        return (q * 2 + m) * rows + (0 if h is None else h * half)

    def token(q, m):
        ahead = CHIP_STEP[q] if isinstance(q, int) else q + lax.div(q, 2) * (5 - 2 * q)
        c = lax.rem(chip + ahead, chips)
        k = core + m - 2 * core * m
        return (c * 2 + k) * rows

    def remote(i, src, dst, to):
        return pltpu.make_async_remote_copy(
            src_ref=src, dst_ref=dst, send_sem=send.at[i], recv_sem=recv.at[i],
            device_id={"tp": to}, device_id_type=MESH)

    def gather_copies(base, own, full):
        blk = lambda q, m: at(full, slot(q, m), rows)
        hlf = lambda q, h: at(full, slot(q, 0, h), half)
        mine = lambda h: at(own, h * half, half)
        copies = {
            POS_A: (mine(0), hlf(LEFT, 0), right),
            POS_B: (mine(1), hlf(LEFT, 1), right),
            NEG_B: (mine(1), hlf(RIGHT, 1), left),
            NEG_A: (mine(0), hlf(RIGHT, 0), left),
            FWD_POS: (hlf(LEFT, 0), hlf(OPP, 0), right),
            FWD_NEG: (hlf(RIGHT, 1), hlf(OPP, 1), left),
            SIB + OWN: (own, blk(OWN, 1), sib),
        }
        for q in (RIGHT, LEFT, OPP):
            copies[SIB + q] = (blk(q, 0), blk(q, 1), sib)
        return {i: remote(base + i, *c) for i, c in copies.items()}

    cdy = gather_copies(0, dy, dyf)
    cx = gather_copies(X0, x, xf)
    csib = [remote(SUM_SIB + q, sibst.at[q % 2], at(sibr, q * rows, rows), sib) for q in range(4)]
    su = lambda i, s, to, dst: remote(i, sumst.at[s], dst, to)
    c2 = [su(U2_POS, 0, right, at(sumr, 0, half)), su(U2_NEG, 1, left, at(sumr, half, half))]
    c1 = [su(U1_POS, 2, right, at(sumr, 2 * half, half)), su(U1_NEG, 3, left, at(sumr, 3 * half, half))]
    c3 = [su(U3_POS, 0, right, last.at[0]), su(U3_NEG, 1, left, last.at[1])]

    barrier = pltpu.get_barrier_semaphore()
    for other in (left, right, sib):
        pl.semaphore_signal(barrier, inc=1, device_id={"tp": other}, device_id_type=MESH)
    pl.semaphore_wait(barrier, 3)

    for i in (POS_A, NEG_B, POS_B, NEG_A, SIB + OWN):
        cdy[i].start()
    cx[SIB + OWN].start()
    weights = [pltpu.make_async_copy(s, t, wsem.at[i]) for i, (s, t) in enumerate(((wd_in, wd), (wg_in, wg), (wu_in, wu)))]
    weights[0].start()

    def load(src, dst, sem):
        return pltpu.make_async_copy(src, dst, sem)

    def start_block(own, full, first, second, q, m, r, b):
        big = act.at[b]
        if own is None:
            load(at(full, slot(q, m), rows), big, lsem.at[b, 0]).start()
        else:
            @pl.when(m == 0)
            def _():
                load(own, big, lsem.at[b, 0]).start()

            @pl.when(m != 0)
            def _():
                load(at(full, slot(q, m), rows), big, lsem.at[b, 0]).start()
        load(at(first, r, rows), gb.at[b], lsem.at[b, 1]).start()
        load(at(second, r, rows), ub.at[b], lsem.at[b, 2]).start()

    def wait_block(b):
        load(dy, act.at[b], lsem.at[b, 0]).wait()
        load(at(gate, 0, rows), gb.at[b], lsem.at[b, 1]).wait()
        load(at(gate, 0, rows), ub.at[b], lsem.at[b, 2]).wait()

    def blocks(count, place, ready, begin, compute):
        ready(0)
        begin(*place(0), 0)

        def body(i, _):
            b = lax.rem(i, 2)
            wait_block(b)

            @pl.when(i + 1 < count)
            def _():
                ready(i + 1)
                begin(*place(i + 1), 1 - b)

            compute(*place(i), b)
            return 0

        lax.fori_loop(0, count, body, 0)

    tile_f = 512 if f % 512 == 0 else f
    tile_d = 512 if d % 512 == 0 else d

    def begin_dy(own):
        return lambda q, m, b: start_block(own, dyf, gate, up, q, m, token(q, m), b)

    def from_dy(q, m, b):
        def columns(j, _):
            c = pl.ds(pl.multiple_of(j * tile_f, tile_f), tile_f)
            d_hidden = dot(act[b], wd[c, :], NT)
            g, u = gb[b, :, c].astype(F32), ub[b, :, c].astype(F32)
            s = lax.logistic(g)
            silu = g * s
            hb[:, c] = (silu * u).astype(BF16)
            dub[:, c] = (d_hidden * silu).astype(BF16)
            t = d_hidden * u
            dgb[:, c] = (t * s + t * g * (s * (1.0 - s))).astype(BF16)
            return 0

        lax.fori_loop(0, f // tile_f, columns, 0)
        r = slot(q, m)
        saves = [load(dgb, at(dgs, r, rows), ssem.at[0]), load(dub, at(dus, r, rows), ssem.at[1])]
        for s in saves:
            s.start()

        def hidden_columns(j, _):
            c = pl.ds(pl.multiple_of(j * tile_f, tile_f), tile_f)
            for k in range(0, d, d // 2):
                accd[c, k : k + d // 2] += dot(hb[:, c], act[b, :, k : k + d // 2], TN)
            return 0

        lax.fori_loop(0, f // tile_f, hidden_columns, 0)
        for s in saves:
            s.wait()

    def begin_x(own):
        return lambda q, m, b: start_block(own, xf, dgs, dus, q, m, slot(q, m), b)

    def from_x(q, m, b):
        def columns(j, _):
            c = pl.ds(pl.multiple_of(j * tile_d, tile_d), tile_d)
            xt = act[b, :, c]
            accg[c, :] += dot(xt, gb[b], TN)
            accu[c, :] += dot(xt, ub[b], TN)
            return 0

        lax.fori_loop(0, d // tile_d, columns, 0)

    def dx_rows(r, count, adds, store):
        loads = [load(at(dgs, r, count), gb.at[0, pl.ds(0, count)], lsem.at[0, 1]), load(at(dus, r, count), ub.at[0, pl.ds(0, count)], lsem.at[0, 2])]
        bufs = [act.at[i, pl.ds(0, count)] for i in range(len(adds))]
        loads += [load(a, t, lsem.at[i, 0]) for i, (a, t) in enumerate(zip(adds, bufs))]
        for o in loads:
            o.start()
        for o in loads:
            o.wait()

        def columns(j, _):
            c = pl.ds(pl.multiple_of(j * tile_d, tile_d), tile_d)
            t = dot(gb[0, :count], wg[c, :], NT) + dot(ub[0, :count], wu[c, :], NT)
            for o in bufs:
                t += o[:, c].astype(F32)
            store(c, t)
            return 0

        lax.fori_loop(0, d // tile_d, columns, 0)

    def dx_for_sibling(q):
        if q >= 2:
            csib[q - 2].wait_send()

        def store(c, t):
            sibst[q % 2, :, c] = t.astype(BF16)

        dx_rows(slot(q, 1), rows, [], store)
        csib[q].start()

    def dx_sum(q, h, s, extra, copy):
        def store(c, t):
            sumst[s, :, c] = t.astype(BF16)

        dx_rows(slot(q, 0, h), half, [at(sibr, q * rows + h * half, half), *extra], store)
        copy.start()

    def zero(ref):
        def body(i, _):
            ref[pl.ds(pl.multiple_of(i * 128, 128), 128), :] = jnp.zeros((128, ref.shape[1]), F32)
            return 0

        lax.fori_loop(0, ref.shape[0] // 128, body, 0)

    nothing = lambda i: None

    def ready_own(copies):
        def ready(i):
            if not isinstance(i, int):
                copies[SIB + OWN].wait_recv()

        return ready

    own_place = lambda i: (0, i)
    weights[1].start()
    weights[2].start()
    for ref in (accd, accg, accu):
        zero(ref)
    weights[0].wait()
    blocks(2, own_place, ready_own(cdy), begin_dy(dy), from_dy)
    weights[1].wait()
    weights[2].wait()
    dx_for_sibling(OWN)

    cdy[POS_A].wait_recv()
    cdy[NEG_B].wait_recv()
    cdy[FWD_POS].start()
    cdy[FWD_NEG].start()
    for i in (POS_A, NEG_B, POS_B, NEG_A):
        cx[i].start()
    blocks(2, own_place, ready_own(cx), begin_x(x), from_x)

    cdy[POS_B].wait_recv()
    cdy[NEG_A].wait_recv()
    cdy[SIB + RIGHT].start()
    cdy[SIB + LEFT].start()

    def ready_near(copies):
        def ready(i):
            if not isinstance(i, int):
                @pl.when(i == 2)
                def _():
                    copies[SIB + RIGHT].wait_recv()
                    copies[SIB + LEFT].wait_recv()

        return ready

    near_place = lambda i: (1 + lax.rem(i, 2), lax.div(i, 2)) if not isinstance(i, int) else (1 + i % 2, i // 2)
    blocks(4, near_place, ready_near(cdy), begin_dy(None), from_dy)
    cdy[FWD_POS].wait_recv()
    cdy[FWD_NEG].wait_recv()
    cdy[SIB + OPP].start()
    dx_for_sibling(RIGHT)
    dx_for_sibling(LEFT)
    csib[RIGHT].wait_recv()
    dx_sum(RIGHT, 1, 0, [], c2[0])
    csib[LEFT].wait_recv()
    dx_sum(LEFT, 0, 1, [], c2[1])

    def ready_far(copies):
        def ready(i):
            if not isinstance(i, int):
                copies[SIB + OPP].wait_recv()

        return ready

    far_place = lambda i: (OPP, i)
    blocks(2, far_place, ready_far(cdy), begin_dy(None), from_dy)
    dx_for_sibling(OPP)
    csib[OPP].wait_recv()
    dx_sum(OPP, 0, 2, [], c1[0])
    dx_sum(OPP, 1, 3, [], c1[1])

    cx[POS_A].wait_recv()
    cx[NEG_B].wait_recv()
    cx[FWD_POS].start()
    cx[FWD_NEG].start()
    cx[POS_B].wait_recv()
    cx[NEG_A].wait_recv()
    cx[SIB + RIGHT].start()
    cx[SIB + LEFT].start()

    csib[LEFT].wait_send()
    csib[OPP].wait_send()
    outs = []
    for i in range(f // rows):
        sibst[i] = accd[i * rows : (i + 1) * rows, :].astype(BF16)
        outs.append(load(sibst.at[i], at(dwd, i * rows, rows), wsem.at[i]))
        outs[-1].start()

    blocks(4, near_place, ready_near(cx), begin_x(None), from_x)

    csib[OWN].wait_recv()
    for h, i in ((1, 0), (0, 1)):
        c2[i].wait_recv()

        def store(c, t, h=h):
            accd[h * half : (h + 1) * half, c] = t

        dx_rows(slot(OWN, 0, h), half, [at(sibr, h * half, half), at(sumr, i * half, half)], store)

    for q, h, i in ((RIGHT, 0, 0), (LEFT, 1, 1)):
        c1[i].wait_recv()
        c2[i].wait_send()
        dx_sum(q, h, i, [at(sumr, (2 + i) * half, half)], c3[i])

    cx[FWD_POS].wait_recv()
    cx[FWD_NEG].wait_recv()
    cx[SIB + OPP].start()
    blocks(2, far_place, ready_far(cx), begin_x(None), from_x)
    for o in outs:
        o.wait()

    outs = []
    for i in range(d // rows):
        b = i % 2
        if i >= 2:
            outs[2 * i - 4].wait()
            outs[2 * i - 3].wait()
        r = slice(i * rows, (i + 1) * rows)
        gb[b] = accg[r, :].astype(BF16)
        outs.append(load(gb.at[b], at(dwg, i * rows, rows), lsem.at[b, 1]))
        outs[-1].start()
        ub[b] = accu[r, :].astype(BF16)
        outs.append(load(ub.at[b], at(dwu, i * rows, rows), lsem.at[b, 2]))
        outs[-1].start()
    for o in outs[-4:]:
        o.wait()

    outs = []
    for i in range(2):
        c3[i].wait_recv()
        r = slice(i * half, (i + 1) * half)
        act[0, r, :] = (accd[r, :] + last[i].astype(F32)).astype(BF16)
        outs.append(load(act.at[0, pl.ds(i * half, half)], at(dx, i * half, half), lsem.at[i, 0]))
        outs[-1].start()
    for o in outs:
        o.wait()
    for c in (*cdy.values(), *cx.values(), *c1, *c3):
        c.wait_send()


def solution(mesh):
    n = mesh.shape["tp"]

    def local(x, dy, gate, up, wg, wu, wd):
        rows, d = x.shape
        tokens, f = gate.shape
        half = rows // 2
        hbm = pl.BlockSpec(memory_space=pltpu.HBM)
        s = lambda *shape: jax.ShapeDtypeStruct(shape, BF16)
        v = lambda *shape: pltpu.VMEM(shape, BF16)
        a = lambda *shape: pltpu.VMEM(shape, F32)
        dma = pltpu.SemaphoreType.DMA
        flops = 12 * tokens * d * f
        outs = pl.pallas_call(
            functools.partial(kernel, n),
            out_shape=(s(rows, d), s(d, f), s(d, f), s(f, d), s(tokens, d), s(tokens, d), s(tokens, f), s(tokens, f), s(4 * rows, d), s(4 * half, d)),
            in_specs=[hbm] * 7,
            out_specs=[hbm] * 10,
            scratch_shapes=[
                v(f, d), v(d, f), v(d, f), a(f, d), a(d, f), a(d, f),
                v(2, rows, d), v(2, rows, f), v(2, rows, f), v(rows, f), v(rows, f), v(rows, f),
                v(2, rows, d), v(4, half, d), v(2, half, d),
                dma((N_COPIES,)), dma((N_COPIES,)), dma((2, 3)), dma((2,)), dma((3,)),
            ],
            compiler_params=pltpu.CompilerParams(collective_id=0, has_side_effects=True, vmem_limit_bytes=67043328),
            cost_estimate=pl.CostEstimate(flops=flops, bytes_accessed=200 * 2**20, transcendentals=tokens * f),
            name="mlp_backward",
        )(x, dy, gate, up, wg, wu, wd)
        return outs[:4]

    rows, columns = P(("dp", "tp"), None), P("dp", "tp")
    return jax.shard_map(
        local,
        mesh=mesh,
        in_specs=(rows, rows, columns, columns, P(None, "tp"), P(None, "tp"), P("tp", None)),
        out_specs=(rows, columns, columns, rows),
        check_vma=False,
    )
```

```python
import functools

import jax
import jax.numpy as jnp
from jax import lax
from jax.experimental import pallas as pl
from jax.experimental.pallas import tpu as pltpu
from jax.sharding import PartitionSpec as P

MESH = pl.DeviceIdType.MESH
NT = (((1,), (1,)), ((), ()))
TN = (((0,), (0,)), ((), ()))
F32, BF16 = jnp.float32, jnp.bfloat16
LIMIT = 41 * 2**20
OWN, RIGHT, LEFT, OPP = range(4)
CHIP_STEP = (0, 1, 3, 2)

POS_A, POS_B, NEG_B, NEG_A, FWD_POS, FWD_NEG, SIB = range(7)
X0 = 10
SUM_SIB = 20
U2_POS, U2_NEG, U1_POS, U1_NEG, U3_POS, U3_NEG = range(24, 30)
N_COPIES = 30


def dot(a, b, dims):
    return lax.dot_general(a, b, dims, preferred_element_type=F32)


def kernel(n, x, dy, gate, up, wg_in, wu_in, wd_in,
           last, wg, wu, sibst, accd, dyf, xf, dgs, dus, sibr, sumr,
           wd, accg, accu, act, gb, ub, dgb, dub, hb, sumst,
           send, recv, lsem, ssem, wsem):
    rows, d = x.shape
    f = gate.shape[1]
    half = rows // 2
    me = lax.axis_index("tp")
    core = lax.rem(me, 2)
    chip = lax.div(me, 2)
    chips = n // 2
    right, left = lax.rem(me + 2, n), lax.rem(me + n - 2, n)
    sib = me + 1 - 2 * core

    def at(ref, start, size):
        if not isinstance(start, int):
            start = pl.multiple_of(start, size)
        return ref.at[pl.ds(start, size)]

    def slot(q, m, h=None):
        return (q * 2 + m) * rows + (0 if h is None else h * half)

    def token(q, m):
        ahead = CHIP_STEP[q] if isinstance(q, int) else q + lax.div(q, 2) * (5 - 2 * q)
        c = lax.rem(chip + ahead, chips)
        k = core + m - 2 * core * m
        return (c * 2 + k) * rows

    def remote(i, src, dst, to):
        return pltpu.make_async_remote_copy(
            src_ref=src, dst_ref=dst, send_sem=send.at[i], recv_sem=recv.at[i],
            device_id={"tp": to}, device_id_type=MESH)

    def gather_copies(base, own, full):
        blk = lambda q, m: at(full, slot(q, m), rows)
        hlf = lambda q, h: at(full, slot(q, 0, h), half)
        mine = lambda h: at(own, h * half, half)
        copies = {
            POS_A: (mine(0), hlf(LEFT, 0), right),
            POS_B: (mine(1), hlf(LEFT, 1), right),
            NEG_B: (mine(1), hlf(RIGHT, 1), left),
            NEG_A: (mine(0), hlf(RIGHT, 0), left),
            FWD_POS: (hlf(LEFT, 0), hlf(OPP, 0), right),
            FWD_NEG: (hlf(RIGHT, 1), hlf(OPP, 1), left),
            SIB + OWN: (own, blk(OWN, 1), sib),
        }
        for q in (RIGHT, LEFT, OPP):
            copies[SIB + q] = (blk(q, 0), blk(q, 1), sib)
        return {i: remote(base + i, *c) for i, c in copies.items()}

    cdy = gather_copies(0, dy, dyf)
    cx = gather_copies(X0, x, xf)
    csib = [remote(SUM_SIB + q, sibst.at[q % 2], at(sibr, q * rows, rows), sib) for q in range(4)]
    su = lambda i, s, to, dst: remote(i, sumst.at[s], dst, to)
    c2 = [su(U2_POS, 0, right, at(sumr, 0, half)), su(U2_NEG, 1, left, at(sumr, half, half))]
    c1 = [su(U1_POS, 2, right, at(sumr, 2 * half, half)), su(U1_NEG, 3, left, at(sumr, 3 * half, half))]
    c3 = [su(U3_POS, 0, right, last.at[0]), su(U3_NEG, 1, left, last.at[1])]

    barrier = pltpu.get_barrier_semaphore()
    for other in (left, right, sib):
        pl.semaphore_signal(barrier, inc=1, device_id={"tp": other}, device_id_type=MESH)
    pl.semaphore_wait(barrier, 3)

    for i in (POS_A, NEG_B, POS_B, NEG_A, SIB + OWN):
        cdy[i].start()
    cx[SIB + OWN].start()
    weights = [pltpu.make_async_copy(s, t, wsem.at[i]) for i, (s, t) in enumerate(((wd_in, wd), (wg_in, wg), (wu_in, wu)))]
    weights[0].start()

    def load(src, dst, sem):
        return pltpu.make_async_copy(src, dst, sem)

    def start_block(own, full, first, second, q, m, r, b):
        big = act.at[b]
        if own is None:
            load(at(full, slot(q, m), rows), big, lsem.at[b, 0]).start()
        else:
            @pl.when(m == 0)
            def _():
                load(own, big, lsem.at[b, 0]).start()

            @pl.when(m != 0)
            def _():
                load(at(full, slot(q, m), rows), big, lsem.at[b, 0]).start()
        load(at(first, r, rows), gb.at[b], lsem.at[b, 1]).start()
        load(at(second, r, rows), ub.at[b], lsem.at[b, 2]).start()

    def wait_block(b):
        load(dy, act.at[b], lsem.at[b, 0]).wait()
        load(at(gate, 0, rows), gb.at[b], lsem.at[b, 1]).wait()
        load(at(gate, 0, rows), ub.at[b], lsem.at[b, 2]).wait()

    def blocks(count, place, ready, begin, compute):
        ready(0)
        begin(*place(0), 0)

        def body(i, _):
            b = lax.rem(i, 2)
            wait_block(b)

            @pl.when(i + 1 < count)
            def _():
                ready(i + 1)
                begin(*place(i + 1), 1 - b)

            compute(*place(i), b)
            return 0

        lax.fori_loop(0, count, body, 0)

    tile_f = 512 if f % 512 == 0 else f
    tile_d = 512 if d % 512 == 0 else d

    def begin_dy(own):
        return lambda q, m, b: start_block(own, dyf, gate, up, q, m, token(q, m), b)

    def from_dy(q, m, b):
        def columns(j, _):
            c = pl.ds(pl.multiple_of(j * tile_f, tile_f), tile_f)
            d_hidden = dot(act[b], wd[c, :], NT)
            g, u = gb[b, :, c].astype(F32), ub[b, :, c].astype(F32)
            s = lax.logistic(g)
            silu = g * s
            hb[:, c] = (silu * u).astype(BF16)
            dub[:, c] = (d_hidden * silu).astype(BF16)
            t = d_hidden * u
            dgb[:, c] = (t * s + t * g * (s * (1.0 - s))).astype(BF16)
            return 0

        lax.fori_loop(0, f // tile_f, columns, 0)
        r = slot(q, m)
        saves = [load(dgb, at(dgs, r, rows), ssem.at[0]), load(dub, at(dus, r, rows), ssem.at[1])]
        for s in saves:
            s.start()

        def hidden_columns(j, _):
            c = pl.ds(pl.multiple_of(j * tile_f, tile_f), tile_f)
            for k in range(0, d, d // 2):
                accd[c, k : k + d // 2] += dot(hb[:, c], act[b, :, k : k + d // 2], TN)
            return 0

        lax.fori_loop(0, f // tile_f, hidden_columns, 0)
        for s in saves:
            s.wait()

    def begin_x(own):
        return lambda q, m, b: start_block(own, xf, dgs, dus, q, m, slot(q, m), b)

    def from_x(q, m, b):
        def columns(j, _):
            c = pl.ds(pl.multiple_of(j * tile_d, tile_d), tile_d)
            xt = act[b, :, c]
            accg[c, :] += dot(xt, gb[b], TN)
            accu[c, :] += dot(xt, ub[b], TN)
            return 0

        lax.fori_loop(0, d // tile_d, columns, 0)

    def dx_rows(r, count, adds, store):
        loads = [load(at(dgs, r, count), gb.at[0, pl.ds(0, count)], lsem.at[0, 1]), load(at(dus, r, count), ub.at[0, pl.ds(0, count)], lsem.at[0, 2])]
        bufs = [act.at[i, pl.ds(0, count)] for i in range(len(adds))]
        loads += [load(a, t, lsem.at[i, 0]) for i, (a, t) in enumerate(zip(adds, bufs))]
        for o in loads:
            o.start()
        for o in loads:
            o.wait()

        def columns(j, _):
            c = pl.ds(pl.multiple_of(j * tile_d, tile_d), tile_d)
            t = dot(gb[0, :count], wg[c, :], NT) + dot(ub[0, :count], wu[c, :], NT)
            for o in bufs:
                t += o[:, c].astype(F32)
            store(c, t)
            return 0

        lax.fori_loop(0, d // tile_d, columns, 0)

    def dx_for_sibling(q):
        if q >= 2:
            csib[q - 2].wait_send()

        def store(c, t):
            sibst[q % 2, :, c] = t.astype(BF16)

        dx_rows(slot(q, 1), rows, [], store)
        csib[q].start()

    def dx_sum(q, h, s, extra, copy):
        def store(c, t):
            sumst[s, :, c] = t.astype(BF16)

        dx_rows(slot(q, 0, h), half, [at(sibr, q * rows + h * half, half), *extra], store)
        copy.start()

    def zero(ref):
        def body(i, _):
            ref[pl.ds(pl.multiple_of(i * 128, 128), 128), :] = jnp.zeros((128, ref.shape[1]), F32)
            return 0

        lax.fori_loop(0, ref.shape[0] // 128, body, 0)

    nothing = lambda i: None

    def ready_own(copies):
        def ready(i):
            if not isinstance(i, int):
                copies[SIB + OWN].wait_recv()

        return ready

    own_place = lambda i: (0, i)
    weights[1].start()
    weights[2].start()
    for ref in (accd, accg, accu):
        zero(ref)
    weights[0].wait()
    blocks(2, own_place, ready_own(cdy), begin_dy(dy), from_dy)
    weights[1].wait()
    weights[2].wait()
    dx_for_sibling(OWN)

    cdy[POS_A].wait_recv()
    cdy[NEG_B].wait_recv()
    cdy[FWD_POS].start()
    cdy[FWD_NEG].start()
    for i in (POS_A, NEG_B, POS_B, NEG_A):
        cx[i].start()
    blocks(2, own_place, ready_own(cx), begin_x(x), from_x)

    cdy[POS_B].wait_recv()
    cdy[NEG_A].wait_recv()
    cdy[SIB + RIGHT].start()
    cdy[SIB + LEFT].start()

    def ready_near(copies):
        def ready(i):
            if not isinstance(i, int):
                @pl.when(i == 2)
                def _():
                    copies[SIB + RIGHT].wait_recv()
                    copies[SIB + LEFT].wait_recv()

        return ready

    near_place = lambda i: (1 + lax.rem(i, 2), lax.div(i, 2)) if not isinstance(i, int) else (1 + i % 2, i // 2)
    blocks(4, near_place, ready_near(cdy), begin_dy(None), from_dy)
    cdy[FWD_POS].wait_recv()
    cdy[FWD_NEG].wait_recv()
    cdy[SIB + OPP].start()
    dx_for_sibling(RIGHT)
    dx_for_sibling(LEFT)
    csib[RIGHT].wait_recv()
    dx_sum(RIGHT, 1, 0, [], c2[0])
    csib[LEFT].wait_recv()
    dx_sum(LEFT, 0, 1, [], c2[1])

    def ready_far(copies):
        def ready(i):
            if not isinstance(i, int):
                copies[SIB + OPP].wait_recv()

        return ready

    far_place = lambda i: (OPP, i)
    blocks(2, far_place, ready_far(cdy), begin_dy(None), from_dy)
    dx_for_sibling(OPP)
    csib[OPP].wait_recv()
    dx_sum(OPP, 0, 2, [], c1[0])
    dx_sum(OPP, 1, 3, [], c1[1])

    cx[POS_A].wait_recv()
    cx[NEG_B].wait_recv()
    cx[FWD_POS].start()
    cx[FWD_NEG].start()
    cx[POS_B].wait_recv()
    cx[NEG_A].wait_recv()
    cx[SIB + RIGHT].start()
    cx[SIB + LEFT].start()

    csib[LEFT].wait_send()
    csib[OPP].wait_send()
    for i in range(f // rows):
        sibst[i] = accd[i * rows : (i + 1) * rows, :].astype(BF16)

    blocks(4, near_place, ready_near(cx), begin_x(None), from_x)

    csib[OWN].wait_recv()
    for h, i in ((1, 0), (0, 1)):
        c2[i].wait_recv()

        def store(c, t, h=h):
            accd[h * half : (h + 1) * half, c] = t

        dx_rows(slot(OWN, 0, h), half, [at(sibr, h * half, half), at(sumr, i * half, half)], store)

    for q, h, i in ((RIGHT, 0, 0), (LEFT, 1, 1)):
        c1[i].wait_recv()
        c2[i].wait_send()
        dx_sum(q, h, i, [at(sumr, (2 + i) * half, half)], c3[i])

    cx[FWD_POS].wait_recv()
    cx[FWD_NEG].wait_recv()
    cx[SIB + OPP].start()
    blocks(2, far_place, ready_far(cx), begin_x(None), from_x)

    for i in range(d // rows):
        r = slice(i * rows, (i + 1) * rows)
        wg[r, :] = accg[r, :].astype(BF16)
        wu[r, :] = accu[r, :].astype(BF16)
    for c in c3:
        c.wait_recv()
    for c in (*cdy.values(), *cx.values(), *c1, *c3):
        c.wait_send()


def finish(last, dwg_in, dwu_in, dwd_in, held, dx, dwg, dwu, dwd, dxb, sem):
    half = last.shape[1]
    rows = 2 * half
    copies = [pltpu.make_async_copy(s, t, sem.at[i]) for i, (s, t) in enumerate(((dwg_in, dwg), (dwu_in, dwu)))]
    copies += [pltpu.make_async_copy(dwd_in.at[i], dwd.at[pl.ds(i * rows, rows)], sem.at[2 + i]) for i in range(dwd_in.shape[0])]
    for c in copies:
        c.start()
    for i in range(2):
        r = slice(i * half, (i + 1) * half)
        dxb[r, :] = (held[r, :] + last[i].astype(F32)).astype(BF16)
    copies.append(pltpu.make_async_copy(dxb, dx, sem.at[len(copies)]))
    copies[-1].start()
    for c in copies:
        c.wait()


def solution(mesh):
    n = mesh.shape["tp"]

    def local(x, dy, gate, up, wg, wu, wd):
        rows, d = x.shape
        tokens, f = gate.shape
        half = rows // 2
        hbm, vmem = pl.BlockSpec(memory_space=pltpu.HBM), pl.BlockSpec(memory_space=pltpu.VMEM)
        s = lambda *shape: jax.ShapeDtypeStruct(shape, BF16)
        v = lambda *shape: pltpu.VMEM(shape, BF16)
        a = lambda *shape: pltpu.VMEM(shape, F32)
        dma = pltpu.SemaphoreType.DMA
        flops = 12 * tokens * d * f
        outs = pl.pallas_call(
            functools.partial(kernel, n),
            out_shape=(
                v(2, half, d), v(d, f), v(d, f), v(f // rows, rows, d), a(f, d),
                s(tokens, d), s(tokens, d), s(tokens, f), s(tokens, f), s(4 * rows, d), s(4 * half, d),
            ),
            in_specs=[hbm] * 7,
            out_specs=[vmem] * 5 + [hbm] * 6,
            scratch_shapes=[
                v(f, d), a(d, f), a(d, f),
                v(2, rows, d), v(2, rows, f), v(2, rows, f), v(rows, f), v(rows, f), v(rows, f), v(4, half, d),
                dma((N_COPIES,)), dma((N_COPIES,)), dma((2, 3)), dma((2,)), dma((3,)),
            ],
            compiler_params=pltpu.CompilerParams(collective_id=0, has_side_effects=True, vmem_limit_bytes=LIMIT),
            cost_estimate=pl.CostEstimate(flops=flops, bytes_accessed=200 * 2**20, transcendentals=tokens * f),
            name="mlp_backward",
        )(x, dy, gate, up, wg, wu, wd)
        return pl.pallas_call(
            finish,
            out_shape=(s(rows, d), s(d, f), s(d, f), s(f, d)),
            in_specs=[vmem] * 5,
            out_specs=[hbm] * 4,
            scratch_shapes=[v(rows, d), dma((3 + f // rows,))],
            compiler_params=pltpu.CompilerParams(vmem_limit_bytes=4 * 2**20),
            name="finish",
        )(*outs[:5])

    rows, columns = P(("dp", "tp"), None), P("dp", "tp")
    return jax.shard_map(
        local,
        mesh=mesh,
        in_specs=(rows, rows, columns, columns, P(None, "tp"), P(None, "tp"), P("tp", None)),
        out_specs=(rows, columns, columns, rows),
        check_vma=False,
    )
```

```python
import functools

import jax
import jax.numpy as jnp
from jax import lax
from jax.experimental import pallas as pl
from jax.experimental.pallas import tpu as pltpu
from jax.sharding import PartitionSpec as P

MESH = pl.DeviceIdType.MESH
NT = (((1,), (1,)), ((), ()))
TN = (((0,), (0,)), ((), ()))
F32, BF16 = jnp.float32, jnp.bfloat16
LIMIT = 41 * 2**20
OWN, RIGHT, LEFT, OPP = range(4)
CHIP_STEP = (0, 1, 3, 2)

POS_A, POS_B, NEG_B, NEG_A, FWD_POS, FWD_NEG, SIB = range(7)
X0 = 10
SUM_SIB = 20
U2_POS, U2_NEG, U1_POS, U1_NEG, U3_POS, U3_NEG = range(24, 30)
N_COPIES = 30


def dot(a, b, dims):
    return lax.dot_general(a, b, dims, preferred_element_type=F32)


def kernel(n, x, dy, gate, up, wg_in, wu_in, wd_in,
           early, passed, wg, wu, sibst, accd, dyf, xf, dgs, dus, sibr, sumr,
           wd, accg, accu, act, gb, ub, dgb, dub, hb, sumst,
           send, recv, lsem, asem, ssem, wsem):
    rows, d = x.shape
    f = gate.shape[1]
    half = rows // 2
    me = lax.axis_index("tp")
    core = lax.rem(me, 2)
    chip = lax.div(me, 2)
    chips = n // 2
    right, left = lax.rem(me + 2, n), lax.rem(me + n - 2, n)
    sib = me + 1 - 2 * core

    def at(ref, start, size):
        if not isinstance(start, int):
            start = pl.multiple_of(start, size)
        return ref.at[pl.ds(start, size)]

    def slot(q, m, h=None):
        return (q * 2 + m) * rows + (0 if h is None else h * half)

    def token(q, m):
        ahead = CHIP_STEP[q] if isinstance(q, int) else q + lax.div(q, 2) * (5 - 2 * q)
        c = lax.rem(chip + ahead, chips)
        k = core + m - 2 * core * m
        return (c * 2 + k) * rows

    def remote(i, src, dst, to):
        return pltpu.make_async_remote_copy(
            src_ref=src, dst_ref=dst, send_sem=send.at[i], recv_sem=recv.at[i],
            device_id={"tp": to}, device_id_type=MESH)

    def gather_copies(base, own, full):
        blk = lambda q, m: at(full, slot(q, m), rows)
        hlf = lambda q, h: at(full, slot(q, 0, h), half)
        mine = lambda h: at(own, h * half, half)
        copies = {
            POS_A: (mine(0), hlf(LEFT, 0), right),
            POS_B: (mine(1), hlf(LEFT, 1), right),
            NEG_B: (mine(1), hlf(RIGHT, 1), left),
            NEG_A: (mine(0), hlf(RIGHT, 0), left),
            FWD_POS: (hlf(LEFT, 0), hlf(OPP, 0), right),
            FWD_NEG: (hlf(RIGHT, 1), hlf(OPP, 1), left),
            SIB + OWN: (own, blk(OWN, 1), sib),
        }
        for q in (RIGHT, LEFT, OPP):
            copies[SIB + q] = (blk(q, 0), blk(q, 1), sib)
        return {i: remote(base + i, *c) for i, c in copies.items()}

    cdy = gather_copies(0, dy, dyf)
    cx = gather_copies(X0, x, xf)
    stage = {OWN: 0, OPP: 1, RIGHT: 0, LEFT: 1}
    csib = [remote(SUM_SIB + q, sibst.at[stage[q]], at(sibr, q * rows, rows), sib) for q in range(4)]
    su = lambda i, s, to, dst: remote(i, sumst.at[s], dst, to)
    c2 = [su(U2_POS, 0, right, at(sumr, 0, half)), su(U2_NEG, 1, left, at(sumr, half, half))]
    c1 = [su(U1_POS, 2, right, at(sumr, 2 * half, half)), su(U1_NEG, 3, left, at(sumr, 3 * half, half))]
    c3 = [remote(i, passed.at[h], early.at[h], to) for i, h, to in ((U3_POS, 0, right), (U3_NEG, 1, left))]

    barrier = pltpu.get_barrier_semaphore()
    for other in (left, right, sib):
        pl.semaphore_signal(barrier, inc=1, device_id={"tp": other}, device_id_type=MESH)
    pl.semaphore_wait(barrier, 3)

    for i in (POS_A, NEG_B, POS_B, NEG_A, SIB + OWN):
        cdy[i].start()
    cx[SIB + OWN].start()
    weights = [pltpu.make_async_copy(s, t, wsem.at[i]) for i, (s, t) in enumerate(((wd_in, wd), (wg_in, wg), (wu_in, wu)))]
    weights[0].start()

    def load(src, dst, sem):
        return pltpu.make_async_copy(src, dst, sem)

    def start_block(own, full, first, second, q, m, r, b):
        big = act.at[b]
        if own is None:
            load(at(full, slot(q, m), rows), big, lsem.at[b, 0]).start()
        else:
            @pl.when(m == 0)
            def _():
                load(own, big, lsem.at[b, 0]).start()

            @pl.when(m != 0)
            def _():
                load(at(full, slot(q, m), rows), big, lsem.at[b, 0]).start()
        load(at(first, r, rows), gb.at[b], lsem.at[b, 1]).start()
        load(at(second, r, rows), ub.at[b], lsem.at[b, 2]).start()

    def wait_block(b):
        load(dy, act.at[b], lsem.at[b, 0]).wait()
        load(at(gate, 0, rows), gb.at[b], lsem.at[b, 1]).wait()
        load(at(gate, 0, rows), ub.at[b], lsem.at[b, 2]).wait()

    def blocks(count, place, ready, begin, compute):
        ready(0)
        begin(*place(0), 0)

        def body(i, _):
            b = lax.rem(i, 2)
            wait_block(b)

            @pl.when(i + 1 < count)
            def _():
                ready(i + 1)
                begin(*place(i + 1), 1 - b)

            compute(*place(i), b)
            return 0

        lax.fori_loop(0, count, body, 0)

    tile_f = 512 if f % 512 == 0 else f
    tile_d = 512 if d % 512 == 0 else d

    def begin_dy(own):
        return lambda q, m, b: start_block(own, dyf, gate, up, q, m, token(q, m), b)

    def from_dy(q, m, b):
        def columns(j, _):
            c = pl.ds(pl.multiple_of(j * tile_f, tile_f), tile_f)
            d_hidden = dot(act[b], wd[c, :], NT)
            g, u = gb[b, :, c].astype(F32), ub[b, :, c].astype(F32)
            s = lax.logistic(g)
            silu = g * s
            hb[:, c] = (silu * u).astype(BF16)
            dub[:, c] = (d_hidden * silu).astype(BF16)
            t = d_hidden * u
            dgb[:, c] = (t * s + t * g * (s * (1.0 - s))).astype(BF16)
            return 0

        lax.fori_loop(0, f // tile_f, columns, 0)
        r = slot(q, m)
        saves = [load(dgb, at(dgs, r, rows), ssem.at[0]), load(dub, at(dus, r, rows), ssem.at[1])]
        for s in saves:
            s.start()

        def hidden_columns(j, _):
            c = pl.ds(pl.multiple_of(j * tile_f, tile_f), tile_f)
            for k in range(0, d, d // 2):
                accd[c, k : k + d // 2] += dot(hb[:, c], act[b, :, k : k + d // 2], TN)
            return 0

        lax.fori_loop(0, f // tile_f, hidden_columns, 0)
        for s in saves:
            s.wait()

    def begin_x(own):
        return lambda q, m, b: start_block(own, xf, dgs, dus, q, m, slot(q, m), b)

    def from_x(q, m, b):
        def columns(j, _):
            c = pl.ds(pl.multiple_of(j * tile_d, tile_d), tile_d)
            xt = act[b, :, c]
            accg[c, :] += dot(xt, gb[b], TN)
            accu[c, :] += dot(xt, ub[b], TN)
            return 0

        lax.fori_loop(0, d // tile_d, columns, 0)

    def dx_jobs(*jobs):
        def loads(k):
            r, count, adds, *_ = jobs[k]
            b = k % 2
            copies = []
            if r is not None:
                copies.append(load(at(dgs, r, count), gb.at[b, pl.ds(0, count)], lsem.at[b, 1]))
                copies.append(load(at(dus, r, count), ub.at[b, pl.ds(0, count)], lsem.at[b, 2]))
            for i, a in enumerate(adds):
                copies.append(load(a, act.at[b, pl.ds(i * half, half)], asem.at[b, i]))
            return copies

        def begin(k):
            for c in jobs[k][3]:
                c.wait_recv()
            for c in loads(k):
                c.start()

        begin(0)
        for k, (r, count, adds, _, store, after) in enumerate(jobs):
            if k + 1 < len(jobs):
                begin(k + 1)
            for c in loads(k):
                c.wait()
            b = k % 2
            g, u = (gb.at[b], ub.at[b]) if r is not None else (dgb, dub)

            def columns(j, _, g=g, u=u, b=b, count=count, adds=adds, store=store):
                c = pl.ds(pl.multiple_of(j * tile_d, tile_d), tile_d)
                t = dot(g[:count, :], wg[c, :], NT) + dot(u[:count, :], wu[c, :], NT)
                for i in range(len(adds)):
                    t += act[b, i * half : (i + 1) * half, c].astype(F32)
                store(c, t)
                return 0

            lax.fori_loop(0, d // tile_d, columns, 0)
            after()

    def put(into):
        def store(c, t):
            into[:, c] = t.astype(BF16)

        return store

    def for_sibling(q, here=False, before=None, after=None):
        def done():
            csib[q].start()
            if before is not None:
                before.wait_send()
            if after is not None:
                after()

        return (None if here else slot(q, 1), rows, [], [], put(sibst.at[stage[q]]), done)

    def chip_sum(q, h, into, extra, ready, after):
        return (slot(q, 0, h), half, [at(sibr, q * rows + h * half, half), *extra], ready, put(into), after)

    def zero(ref):
        def body(i, _):
            ref[pl.ds(pl.multiple_of(i * 128, 128), 128), :] = jnp.zeros((128, ref.shape[1]), F32)
            return 0

        lax.fori_loop(0, ref.shape[0] // 128, body, 0)

    nothing = lambda i: None

    def ready_own(copies):
        def ready(i):
            if not isinstance(i, int):
                copies[SIB + OWN].wait_recv()

        return ready

    own_place = lambda i: (0, i)
    weights[1].start()
    weights[2].start()
    for ref in (accd, accg, accu):
        zero(ref)
    weights[0].wait()
    blocks(2, own_place, ready_own(cdy), begin_dy(dy), from_dy)
    weights[1].wait()
    weights[2].wait()
    dx_jobs(for_sibling(OWN, here=True))

    cdy[POS_A].wait_recv()
    cdy[NEG_B].wait_recv()
    cdy[FWD_POS].start()
    cdy[FWD_NEG].start()
    for i in (POS_A, NEG_B, POS_B, NEG_A):
        cx[i].start()
    blocks(2, own_place, ready_own(cx), begin_x(x), from_x)

    cdy[POS_B].wait_recv()
    cdy[NEG_A].wait_recv()
    cdy[SIB + RIGHT].start()
    cdy[SIB + LEFT].start()

    def ready_near(copies):
        def ready(i):
            if not isinstance(i, int):
                @pl.when(i == 2)
                def _():
                    copies[SIB + RIGHT].wait_recv()
                    copies[SIB + LEFT].wait_recv()

        return ready

    near_place = lambda i: (1 + lax.rem(i, 2), lax.div(i, 2)) if not isinstance(i, int) else (1 + i % 2, i // 2)
    blocks(4, near_place, ready_near(cdy), begin_dy(None), from_dy)
    cdy[FWD_POS].wait_recv()
    cdy[FWD_NEG].wait_recv()
    cdy[SIB + OPP].start()

    def ready_far(copies):
        def ready(i):
            if not isinstance(i, int):
                copies[SIB + OPP].wait_recv()

        return ready

    far_place = lambda i: (OPP, i)
    blocks(2, far_place, ready_far(cdy), begin_dy(None), from_dy)

    def forward_x():
        cx[POS_A].wait_recv()
        cx[NEG_B].wait_recv()
        cx[FWD_POS].start()
        cx[FWD_NEG].start()

    dx_jobs(
        for_sibling(OPP, here=True, before=csib[OWN]),
        for_sibling(RIGHT, before=csib[OPP], after=forward_x),
        for_sibling(LEFT),
        chip_sum(OPP, 0, sumst.at[2], [], [csib[OPP]], c1[0].start),
        chip_sum(OPP, 1, sumst.at[3], [], [], c1[1].start),
        chip_sum(RIGHT, 1, sumst.at[0], [], [csib[RIGHT]], c2[0].start),
        chip_sum(LEFT, 0, sumst.at[1], [], [csib[LEFT]], c2[1].start),
    )

    cx[POS_B].wait_recv()
    cx[NEG_A].wait_recv()
    cx[SIB + RIGHT].start()
    cx[SIB + LEFT].start()

    csib[RIGHT].wait_send()
    csib[LEFT].wait_send()
    for i in range(f // rows):
        sibst[i] = accd[i * rows : (i + 1) * rows, :].astype(BF16)

    blocks(4, near_place, ready_near(cx), begin_x(None), from_x)


    def hold(h):
        def store(c, t):
            accd[h * half : (h + 1) * half, c] = t

        ready = [csib[OWN]] if h == 0 else []
        return (slot(OWN, 0, h), half, [at(sibr, h * half, half)], ready, store, lambda: None)

    dx_jobs(hold(0), hold(1))

    cx[FWD_POS].wait_recv()
    cx[FWD_NEG].wait_recv()
    cx[SIB + OPP].start()
    blocks(2, far_place, ready_far(cx), begin_x(None), from_x)

    def passing(i, q, h):
        def after():
            @pl.when(core == 1)
            def _():
                c3[i].start()

        return chip_sum(q, h, passed.at[i], [at(sumr, (2 + i) * half, half)], [c1[i]], after)

    dx_jobs(passing(0, RIGHT, 0), passing(1, LEFT, 1))

    for i in range(d // rows):
        r = slice(i * rows, (i + 1) * rows)
        wg[r, :] = accg[r, :].astype(BF16)
        wu[r, :] = accu[r, :].astype(BF16)
    for c in c2:
        c.wait_recv()
    for c in (*cdy.values(), *cx.values(), *c1, *c2):
        c.wait_send()

    @pl.when(core == 1)
    def _():
        for c in c3:
            c.wait_recv()
            c.wait_send()


def write_weights(dwg_in, dwu_in, dwd_in, own, sumr, early, held, dwg, dwu, dwd, token, near, sem):
    core = lax.rem(lax.axis_index("tp"), 2)
    half = near.shape[1]
    rows = 2 * half
    adds = [pltpu.make_async_copy(sumr.at[pl.ds((1 - h) * half, half)], near.at[h], sem.at[h]) for h in range(2)]
    more = [pltpu.make_async_copy(early.at[h], near.at[2 + h], sem.at[2 + h]) for h in range(2)]
    copies = [pltpu.make_async_copy(s, t, sem.at[4 + i]) for i, (s, t) in enumerate(((dwg_in, dwg), (dwu_in, dwu)))]
    copies += [pltpu.make_async_copy(dwd_in.at[i], dwd.at[pl.ds(i * rows, rows)], sem.at[6 + i]) for i in range(dwd_in.shape[0])]
    for c in (*adds, *copies):
        c.start()
    token[...] = jnp.zeros_like(token)

    @pl.when(core == 1)
    def _():
        for c in more:
            c.start()

    for h in range(2):
        adds[h].wait()
        r = slice(h * half, (h + 1) * half)
        held[r, :] = own[r, :] + near[h].astype(F32)

    @pl.when(core == 1)
    def _():
        for h in range(2):
            more[h].wait()
            r = slice(h * half, (h + 1) * half)
            held[r, :] += near[2 + h].astype(F32)

    for c in copies:
        c.wait()


def pass_on(n, passed, token, late, send, recv):
    me = lax.axis_index("tp")
    core = lax.rem(me, 2)
    right, left = lax.rem(me + 2, n), lax.rem(me + n - 2, n)
    half = passed.shape[1]
    barrier = pltpu.get_barrier_semaphore()
    for other in (left, right):
        pl.semaphore_signal(barrier, inc=1, device_id={"tp": other}, device_id_type=MESH)
    pl.semaphore_wait(barrier, 2)

    @pl.when(core == 0)
    def _():
        copies = [
            pltpu.make_async_remote_copy(
                src_ref=passed.at[h], dst_ref=late.at[h], send_sem=send.at[h], recv_sem=recv.at[h],
                device_id={"tp": to}, device_id_type=MESH)
            for h, to in enumerate((right, left))
        ]
        for c in copies:
            c.start()
        for c in copies:
            c.wait()


def finish(held, late, dx, dxb, sem):
    core = lax.rem(lax.axis_index("tp"), 2)
    half = late.shape[1]
    copies = []
    for h in range(2):
        r = pl.ds(h * half, half)

        @pl.when(core == 0)
        def _(r=r, h=h):
            dxb[r, :] = (held[r, :] + late[h].astype(F32)).astype(BF16)

        @pl.when(core == 1)
        def _(r=r):
            dxb[r, :] = held[r, :].astype(BF16)

        copies.append(pltpu.make_async_copy(dxb.at[r], dx.at[r], sem.at[h]))
        copies[-1].start()
    for c in copies:
        c.wait()


def solution(mesh):
    n = mesh.shape["tp"]

    def local(x, dy, gate, up, wg, wu, wd):
        rows, d = x.shape
        tokens, f = gate.shape
        half = rows // 2
        hbm, vmem = pl.BlockSpec(memory_space=pltpu.HBM), pl.BlockSpec(memory_space=pltpu.VMEM)
        s = lambda *shape: jax.ShapeDtypeStruct(shape, BF16)
        v = lambda *shape: pltpu.VMEM(shape, BF16)
        a = lambda *shape: pltpu.VMEM(shape, F32)
        dma = pltpu.SemaphoreType.DMA
        flops = 12 * tokens * d * f
        early, passed, dwg, dwu, dwd, own, *_, sumr = pl.pallas_call(
            functools.partial(kernel, n),
            out_shape=(
                pltpu.HBM((2, half, d), BF16), v(2, half, d), v(d, f), v(d, f), v(f // rows, rows, d), a(f, d),
                s(tokens, d), s(tokens, d), s(tokens, f), s(tokens, f), s(4 * rows, d), pltpu.HBM((4 * half, d), BF16),
            ),
            in_specs=[hbm] * 7,
            out_specs=[hbm] + [vmem] * 5 + [hbm] * 6,
            scratch_shapes=[
                v(f, d), a(d, f), a(d, f),
                v(2, rows, d), v(2, rows, f), v(2, rows, f), v(rows, f), v(rows, f), v(rows, f), v(4, half, d),
                dma((N_COPIES,)), dma((N_COPIES,)), dma((2, 3)), dma((2, 2)), dma((2,)), dma((3,)),
            ],
            compiler_params=pltpu.CompilerParams(collective_id=0, has_side_effects=True, vmem_limit_bytes=LIMIT),
            cost_estimate=pl.CostEstimate(flops=flops, bytes_accessed=200 * 2**20, transcendentals=tokens * f),
            name="mlp_backward",
        )(x, dy, gate, up, wg, wu, wd)
        in_vmem = lambda t: pltpu.with_memory_space_constraint(t, pltpu.VMEM)
        small = pltpu.CompilerParams(vmem_limit_bytes=8 * 2**20)
        held, dwg, dwu, dwd, token = pl.pallas_call(
            write_weights,
            out_shape=(a(rows, d), s(d, f), s(d, f), s(f, d), v(8, 128)),
            in_specs=[vmem] * 4 + [hbm] * 2,
            out_specs=[vmem, hbm, hbm, hbm, vmem],
            scratch_shapes=[v(4, half, d), dma((6 + f // rows,))],
            compiler_params=small,
            name="write_weights",
        )(*map(in_vmem, (dwg, dwu, dwd, own)), *(pltpu.with_memory_space_constraint(t, pltpu.HBM) for t in (sumr, early)))
        late = pl.pallas_call(
            functools.partial(pass_on, n),
            out_shape=v(2, half, d),
            in_specs=[vmem] * 2,
            out_specs=vmem,
            scratch_shapes=[dma((2,)), dma((2,))],
            compiler_params=pltpu.CompilerParams(collective_id=1, has_side_effects=True, vmem_limit_bytes=8 * 2**20),
            name="pass_on",
        )(in_vmem(passed), in_vmem(token))
        dx = pl.pallas_call(
            finish,
            out_shape=s(rows, d),
            in_specs=[vmem] * 2,
            out_specs=hbm,
            scratch_shapes=[v(rows, d), dma((2,))],
            compiler_params=small,
            name="finish",
        )(*map(in_vmem, (held, late)))
        return dx, dwg, dwu, dwd

    rows, columns = P(("dp", "tp"), None), P("dp", "tp")
    return jax.shard_map(
        local,
        mesh=mesh,
        in_specs=(rows, rows, columns, columns, P(None, "tp"), P(None, "tp"), P("tp", None)),
        out_specs=(rows, columns, columns, rows),
        check_vma=False,
    )
```

```python
import functools

import jax
import jax.numpy as jnp
from jax import lax
from jax.experimental import pallas as pl
from jax.experimental.pallas import tpu as pltpu
from jax.sharding import PartitionSpec as P

MESH = pl.DeviceIdType.MESH
NT = (((1,), (1,)), ((), ()))
TN = (((0,), (0,)), ((), ()))
F32, BF16 = jnp.float32, jnp.bfloat16
LIMIT = 41 * 2**20
LATE = 0
OWN, RIGHT, LEFT, OPP = range(4)
CHIP_STEP = (0, 1, 3, 2)

POS_A, POS_B, NEG_B, NEG_A, FWD_POS, FWD_NEG, SIB = range(7)
X0 = 10
SUM_SIB = 20
U2_POS, U2_NEG, U1_POS, U1_NEG, U3_POS, U3_NEG = range(24, 30)
N_COPIES = 30


def dot(a, b, dims):
    return lax.dot_general(a, b, dims, preferred_element_type=F32)


def kernel(n, x, dy, gate, up, wg_in, wu_in, wd_in,
           early, passed, wg, wu, sibst, accd, dyf, xf, dgs, dus, sibr, sumr,
           wd, accg, accu, act, gb, ub, dgb, dub, hb, sumst,
           send, recv, lsem, asem, ssem, wsem):
    rows, d = x.shape
    f = gate.shape[1]
    half = rows // 2
    me = lax.axis_index("tp")
    core = lax.rem(me, 2)
    chip = lax.div(me, 2)
    chips = n // 2
    right, left = lax.rem(me + 2, n), lax.rem(me + n - 2, n)
    sib = me + 1 - 2 * core

    def at(ref, start, size):
        if not isinstance(start, int):
            start = pl.multiple_of(start, size)
        return ref.at[pl.ds(start, size)]

    def slot(q, m, h=None):
        return (q * 2 + m) * rows + (0 if h is None else h * half)

    def token(q, m):
        ahead = CHIP_STEP[q] if isinstance(q, int) else q + lax.div(q, 2) * (5 - 2 * q)
        c = lax.rem(chip + ahead, chips)
        k = core + m - 2 * core * m
        return (c * 2 + k) * rows

    def remote(i, src, dst, to):
        return pltpu.make_async_remote_copy(
            src_ref=src, dst_ref=dst, send_sem=send.at[i], recv_sem=recv.at[i],
            device_id={"tp": to}, device_id_type=MESH)

    def gather_copies(base, own, full):
        blk = lambda q, m: at(full, slot(q, m), rows)
        hlf = lambda q, h: at(full, slot(q, 0, h), half)
        mine = lambda h: at(own, h * half, half)
        copies = {
            POS_A: (mine(0), hlf(LEFT, 0), right),
            POS_B: (mine(1), hlf(LEFT, 1), right),
            NEG_B: (mine(1), hlf(RIGHT, 1), left),
            NEG_A: (mine(0), hlf(RIGHT, 0), left),
            FWD_POS: (hlf(LEFT, 0), hlf(OPP, 0), right),
            FWD_NEG: (hlf(RIGHT, 1), hlf(OPP, 1), left),
            SIB + OWN: (own, blk(OWN, 1), sib),
        }
        for q in (RIGHT, LEFT, OPP):
            copies[SIB + q] = (blk(q, 0), blk(q, 1), sib)
        return {i: remote(base + i, *c) for i, c in copies.items()}

    cdy = gather_copies(0, dy, dyf)
    cx = gather_copies(X0, x, xf)
    stage = {OWN: 0, OPP: 1, RIGHT: 0, LEFT: 1}
    csib = [remote(SUM_SIB + q, sibst.at[stage[q]], at(sibr, q * rows, rows), sib) for q in range(4)]
    su = lambda i, s, to, dst: remote(i, sumst.at[s], dst, to)
    c2 = [su(U2_POS, 0, right, at(sumr, 0, half)), su(U2_NEG, 1, left, at(sumr, half, half))]
    c1 = [su(U1_POS, 2, right, at(sumr, 2 * half, half)), su(U1_NEG, 3, left, at(sumr, 3 * half, half))]
    c3 = [remote(i, passed.at[h], early.at[h], to) for i, h, to in ((U3_POS, 0, right), (U3_NEG, 1, left))]

    barrier = pltpu.get_barrier_semaphore()
    for other in (left, right, sib):
        pl.semaphore_signal(barrier, inc=1, device_id={"tp": other}, device_id_type=MESH)
    pl.semaphore_wait(barrier, 3)

    for i in (POS_A, NEG_B, POS_B, NEG_A, SIB + OWN):
        cdy[i].start()
    cx[SIB + OWN].start()
    weights = [pltpu.make_async_copy(s, t, wsem.at[i]) for i, (s, t) in enumerate(((wd_in, wd), (wg_in, wg), (wu_in, wu)))]
    weights[0].start()

    def load(src, dst, sem):
        return pltpu.make_async_copy(src, dst, sem)

    def start_block(own, full, first, second, q, m, r, b):
        big = act.at[b]
        if own is None:
            load(at(full, slot(q, m), rows), big, lsem.at[b, 0]).start()
        else:
            @pl.when(m == 0)
            def _():
                load(own, big, lsem.at[b, 0]).start()

            @pl.when(m != 0)
            def _():
                load(at(full, slot(q, m), rows), big, lsem.at[b, 0]).start()
        load(at(first, r, rows), gb.at[b], lsem.at[b, 1]).start()
        load(at(second, r, rows), ub.at[b], lsem.at[b, 2]).start()

    def wait_block(b):
        load(dy, act.at[b], lsem.at[b, 0]).wait()
        load(at(gate, 0, rows), gb.at[b], lsem.at[b, 1]).wait()
        load(at(gate, 0, rows), ub.at[b], lsem.at[b, 2]).wait()

    def blocks(count, place, ready, begin, compute):
        ready(0)
        begin(*place(0), 0)

        def body(i, _):
            b = lax.rem(i, 2)
            wait_block(b)

            @pl.when(i + 1 < count)
            def _():
                ready(i + 1)
                begin(*place(i + 1), 1 - b)

            compute(*place(i), b)
            return 0

        lax.fori_loop(0, count, body, 0)

    tile_f = 512 if f % 512 == 0 else f
    tile_d = 512 if d % 512 == 0 else d

    def begin_dy(own):
        return lambda q, m, b: start_block(own, dyf, gate, up, q, m, token(q, m), b)

    def from_dy(q, m, b):
        def columns(j, _):
            c = pl.ds(pl.multiple_of(j * tile_f, tile_f), tile_f)
            d_hidden = dot(act[b], wd[c, :], NT)
            g, u = gb[b, :, c].astype(F32), ub[b, :, c].astype(F32)
            s = lax.logistic(g)
            silu = g * s
            hb[:, c] = (silu * u).astype(BF16)
            dub[:, c] = (d_hidden * silu).astype(BF16)
            t = d_hidden * u
            dgb[:, c] = (t * s + t * g * (s * (1.0 - s))).astype(BF16)
            return 0

        lax.fori_loop(0, f // tile_f, columns, 0)
        r = slot(q, m)
        saves = [load(dgb, at(dgs, r, rows), ssem.at[0]), load(dub, at(dus, r, rows), ssem.at[1])]
        for s in saves:
            s.start()

        def hidden_columns(j, _):
            c = pl.ds(pl.multiple_of(j * tile_f, tile_f), tile_f)
            for k in range(0, d, d // 2):
                accd[c, k : k + d // 2] += dot(hb[:, c], act[b, :, k : k + d // 2], TN)
            return 0

        lax.fori_loop(0, f // tile_f, hidden_columns, 0)
        for s in saves:
            s.wait()

    def begin_x(own):
        return lambda q, m, b: start_block(own, xf, dgs, dus, q, m, slot(q, m), b)

    def from_x(q, m, b):
        def columns(j, _):
            c = pl.ds(pl.multiple_of(j * tile_d, tile_d), tile_d)
            xt = act[b, :, c]
            accg[c, :] += dot(xt, gb[b], TN)
            accu[c, :] += dot(xt, ub[b], TN)
            return 0

        lax.fori_loop(0, d // tile_d, columns, 0)

    def dx_jobs(*jobs):
        def loads(k):
            r, count, adds, *_ = jobs[k]
            b = k % 2
            copies = []
            if r is not None:
                copies.append(load(at(dgs, r, count), gb.at[b, pl.ds(0, count)], lsem.at[b, 1]))
                copies.append(load(at(dus, r, count), ub.at[b, pl.ds(0, count)], lsem.at[b, 2]))
            for i, a in enumerate(adds):
                copies.append(load(a, act.at[b, pl.ds(i * half, half)], asem.at[b, i]))
            return copies

        def begin(k):
            for c in jobs[k][3]:
                c.wait_recv()
            for c in loads(k):
                c.start()

        begin(0)
        for k, (r, count, adds, _, store, after) in enumerate(jobs):
            if k + 1 < len(jobs):
                begin(k + 1)
            for c in loads(k):
                c.wait()
            b = k % 2
            g, u = (gb.at[b], ub.at[b]) if r is not None else (dgb, dub)

            def columns(j, _, g=g, u=u, b=b, count=count, adds=adds, store=store):
                c = pl.ds(pl.multiple_of(j * tile_d, tile_d), tile_d)
                t = dot(g[:count, :], wg[c, :], NT) + dot(u[:count, :], wu[c, :], NT)
                for i in range(len(adds)):
                    t += act[b, i * half : (i + 1) * half, c].astype(F32)
                store(c, t)
                return 0

            lax.fori_loop(0, d // tile_d, columns, 0)
            after()

    def put(into):
        def store(c, t):
            into[:, c] = t.astype(BF16)

        return store

    def for_sibling(q, here=False, before=None, after=None):
        def done():
            csib[q].start()
            if before is not None:
                before.wait_send()
            if after is not None:
                after()

        return (None if here else slot(q, 1), rows, [], [], put(sibst.at[stage[q]]), done)

    def chip_sum(q, h, into, extra, ready, after):
        return (slot(q, 0, h), half, [at(sibr, q * rows + h * half, half), *extra], ready, put(into), after)

    def zero(ref):
        def body(i, _):
            ref[pl.ds(pl.multiple_of(i * 128, 128), 128), :] = jnp.zeros((128, ref.shape[1]), F32)
            return 0

        lax.fori_loop(0, ref.shape[0] // 128, body, 0)

    nothing = lambda i: None

    def ready_own(copies):
        def ready(i):
            if not isinstance(i, int):
                copies[SIB + OWN].wait_recv()

        return ready

    own_place = lambda i: (0, i)
    weights[1].start()
    weights[2].start()
    for ref in (accd, accg, accu):
        zero(ref)
    weights[0].wait()
    blocks(2, own_place, ready_own(cdy), begin_dy(dy), from_dy)
    weights[1].wait()
    weights[2].wait()
    dx_jobs(for_sibling(OWN, here=True))

    cdy[POS_A].wait_recv()
    cdy[NEG_B].wait_recv()
    cdy[FWD_POS].start()
    cdy[FWD_NEG].start()
    for i in (POS_A, NEG_B, POS_B, NEG_A):
        cx[i].start()
    blocks(2, own_place, ready_own(cx), begin_x(x), from_x)

    cdy[POS_B].wait_recv()
    cdy[NEG_A].wait_recv()
    cdy[SIB + RIGHT].start()
    cdy[SIB + LEFT].start()

    def ready_near(copies):
        def ready(i):
            if not isinstance(i, int):
                @pl.when(i == 2)
                def _():
                    copies[SIB + RIGHT].wait_recv()
                    copies[SIB + LEFT].wait_recv()

        return ready

    near_place = lambda i: (1 + lax.rem(i, 2), lax.div(i, 2)) if not isinstance(i, int) else (1 + i % 2, i // 2)
    blocks(4, near_place, ready_near(cdy), begin_dy(None), from_dy)
    cdy[FWD_POS].wait_recv()
    cdy[FWD_NEG].wait_recv()
    cdy[SIB + OPP].start()

    def ready_far(copies):
        def ready(i):
            if not isinstance(i, int):
                copies[SIB + OPP].wait_recv()

        return ready

    far_place = lambda i: (OPP, i)
    blocks(2, far_place, ready_far(cdy), begin_dy(None), from_dy)

    def forward_x():
        cx[POS_A].wait_recv()
        cx[NEG_B].wait_recv()
        cx[FWD_POS].start()
        cx[FWD_NEG].start()

    dx_jobs(
        for_sibling(OPP, here=True, before=csib[OWN]),
        for_sibling(RIGHT, before=csib[OPP], after=forward_x),
        for_sibling(LEFT),
        chip_sum(OPP, 0, sumst.at[2], [], [csib[OPP]], c1[0].start),
        chip_sum(OPP, 1, sumst.at[3], [], [], c1[1].start),
        chip_sum(RIGHT, 1, sumst.at[0], [], [csib[RIGHT]], c2[0].start),
        chip_sum(LEFT, 0, sumst.at[1], [], [csib[LEFT]], c2[1].start),
    )

    cx[POS_B].wait_recv()
    cx[NEG_A].wait_recv()
    cx[SIB + RIGHT].start()
    cx[SIB + LEFT].start()

    csib[RIGHT].wait_send()
    csib[LEFT].wait_send()
    for i in range(f // rows):
        sibst[i] = accd[i * rows : (i + 1) * rows, :].astype(BF16)

    blocks(4, near_place, ready_near(cx), begin_x(None), from_x)


    def hold(h):
        def store(c, t):
            accd[h * half : (h + 1) * half, c] = t

        ready = [csib[OWN]] if h == 0 else []
        return (slot(OWN, 0, h), half, [at(sibr, h * half, half)], ready, store, lambda: None)

    dx_jobs(hold(0), hold(1))

    cx[FWD_POS].wait_recv()
    cx[FWD_NEG].wait_recv()
    cx[SIB + OPP].start()
    blocks(2, far_place, ready_far(cx), begin_x(None), from_x)

    def passing(i, q, h):
        def after():
            @pl.when(core != LATE)
            def _():
                c3[i].start()

        return chip_sum(q, h, passed.at[i], [at(sumr, (2 + i) * half, half)], [c1[i]], after)

    dx_jobs(passing(0, RIGHT, 0), passing(1, LEFT, 1))

    for i in range(d // rows):
        r = slice(i * rows, (i + 1) * rows)
        wg[r, :] = accg[r, :].astype(BF16)
        wu[r, :] = accu[r, :].astype(BF16)
    for c in c2:
        c.wait_recv()
    for c in (*cdy.values(), *cx.values(), *c1, *c2):
        c.wait_send()

    @pl.when(core != LATE)
    def _():
        for c in c3:
            c.wait_recv()
            c.wait_send()


def write_weights(dwg_in, dwu_in, dwd_in, own, sumr, early, held, dwg, dwu, dwd, token, near, sem):
    core = lax.rem(lax.axis_index("tp"), 2)
    half = near.shape[1]
    rows = 2 * half
    adds = [pltpu.make_async_copy(sumr.at[pl.ds((1 - h) * half, half)], near.at[h], sem.at[h]) for h in range(2)]
    more = [pltpu.make_async_copy(early.at[h], near.at[2 + h], sem.at[2 + h]) for h in range(2)]
    copies = [pltpu.make_async_copy(s, t, sem.at[4 + i]) for i, (s, t) in enumerate(((dwg_in, dwg), (dwu_in, dwu)))]
    copies += [pltpu.make_async_copy(dwd_in.at[i], dwd.at[pl.ds(i * rows, rows)], sem.at[6 + i]) for i in range(dwd_in.shape[0])]
    for c in (*adds, *copies):
        c.start()
    token[...] = jnp.zeros_like(token)

    @pl.when(core != LATE)
    def _():
        for c in more:
            c.start()

    for h in range(2):
        adds[h].wait()
        r = slice(h * half, (h + 1) * half)
        held[r, :] = own[r, :] + near[h].astype(F32)

    @pl.when(core != LATE)
    def _():
        for h in range(2):
            more[h].wait()
            r = slice(h * half, (h + 1) * half)
            held[r, :] += near[2 + h].astype(F32)

    for c in copies:
        c.wait()


def pass_on(n, passed, held, token, dx, late, send, recv):
    me = lax.axis_index("tp")
    core = lax.rem(me, 2)
    right, left = lax.rem(me + 2, n), lax.rem(me + n - 2, n)
    half = passed.shape[1]
    barrier = pltpu.get_barrier_semaphore()
    for other in (left, right):
        pl.semaphore_signal(barrier, inc=1, device_id={"tp": other}, device_id_type=MESH)
    pl.semaphore_wait(barrier, 2)

    @pl.when(core == LATE)
    def _():
        copies = []
        for k, (start, count) in enumerate(((0, half - half // 8), (half - half // 8, half // 8))):
            for h, to in enumerate((right, left)):
                r = pl.ds(start, count)
                c = pltpu.make_async_remote_copy(
                    src_ref=passed.at[h, r], dst_ref=late.at[h, r], send_sem=send.at[h, k], recv_sem=recv.at[h, k],
                    device_id={"tp": to}, device_id_type=MESH)
                c.start()
                copies.append((c, h, start, count))
        for c, h, start, count in copies:
            c.wait_recv()
            r = slice(h * half + start, h * half + start + count)
            dx[r, :] = (held[r, :] + late[h, start : start + count, :].astype(F32)).astype(BF16)
        for c, *_ in copies:
            c.wait_send()

    @pl.when(core != LATE)
    def _():
        dx[...] = held[...].astype(BF16)


def finish(dx_in, dx, sem):
    parts = sem.shape[0]
    count = dx.shape[0] // parts
    copies = [pltpu.make_async_copy(dx_in.at[r], dx.at[r], sem.at[i]) for i in range(parts) for r in (pl.ds(i * count, count),)]
    for c in copies:
        c.start()
    for c in copies:
        c.wait()


def solution(mesh):
    n = mesh.shape["tp"]

    def local(x, dy, gate, up, wg, wu, wd):
        rows, d = x.shape
        tokens, f = gate.shape
        half = rows // 2
        hbm, vmem = pl.BlockSpec(memory_space=pltpu.HBM), pl.BlockSpec(memory_space=pltpu.VMEM)
        s = lambda *shape: jax.ShapeDtypeStruct(shape, BF16)
        v = lambda *shape: pltpu.VMEM(shape, BF16)
        a = lambda *shape: pltpu.VMEM(shape, F32)
        dma = pltpu.SemaphoreType.DMA
        flops = 12 * tokens * d * f
        early, passed, dwg, dwu, dwd, own, *_, sumr = pl.pallas_call(
            functools.partial(kernel, n),
            out_shape=(
                pltpu.HBM((2, half, d), BF16), v(2, half, d), v(d, f), v(d, f), v(f // rows, rows, d), a(f, d),
                s(tokens, d), s(tokens, d), s(tokens, f), s(tokens, f), s(4 * rows, d), pltpu.HBM((4 * half, d), BF16),
            ),
            in_specs=[hbm] * 7,
            out_specs=[hbm] + [vmem] * 5 + [hbm] * 6,
            scratch_shapes=[
                v(f, d), a(d, f), a(d, f),
                v(2, rows, d), v(2, rows, f), v(2, rows, f), v(rows, f), v(rows, f), v(rows, f), v(4, half, d),
                dma((N_COPIES,)), dma((N_COPIES,)), dma((2, 3)), dma((2, 2)), dma((2,)), dma((3,)),
            ],
            compiler_params=pltpu.CompilerParams(collective_id=0, has_side_effects=True, vmem_limit_bytes=LIMIT),
            cost_estimate=pl.CostEstimate(flops=flops, bytes_accessed=200 * 2**20, transcendentals=tokens * f),
            name="mlp_backward",
        )(x, dy, gate, up, wg, wu, wd)
        in_vmem = lambda t: pltpu.with_memory_space_constraint(t, pltpu.VMEM)
        small = pltpu.CompilerParams(vmem_limit_bytes=8 * 2**20)
        held, dwg, dwu, dwd, token = pl.pallas_call(
            write_weights,
            out_shape=(a(rows, d), s(d, f), s(d, f), s(f, d), v(8, 128)),
            in_specs=[vmem] * 4 + [hbm] * 2,
            out_specs=[vmem, hbm, hbm, hbm, vmem],
            scratch_shapes=[v(4, half, d), dma((6 + f // rows,))],
            compiler_params=small,
            name="write_weights",
        )(*map(in_vmem, (dwg, dwu, dwd, own)), *(pltpu.with_memory_space_constraint(t, pltpu.HBM) for t in (sumr, early)))
        dx = pl.pallas_call(
            functools.partial(pass_on, n),
            out_shape=v(rows, d),
            in_specs=[vmem] * 3,
            out_specs=vmem,
            scratch_shapes=[v(2, half, d), dma((2, 2)), dma((2, 2))],
            compiler_params=pltpu.CompilerParams(collective_id=1, has_side_effects=True, vmem_limit_bytes=8 * 2**20),
            name="pass_on",
        )(*map(in_vmem, (passed, held, token)))
        dx = pl.pallas_call(
            finish,
            out_shape=s(rows, d),
            in_specs=[vmem],
            out_specs=hbm,
            scratch_shapes=[dma((1,))],
            compiler_params=small,
            name="finish",
        )(in_vmem(dx))
        return dx, dwg, dwu, dwd

    rows, columns = P(("dp", "tp"), None), P("dp", "tp")
    return jax.shard_map(
        local,
        mesh=mesh,
        in_specs=(rows, rows, columns, columns, P(None, "tp"), P(None, "tp"), P("tp", None)),
        out_specs=(rows, columns, columns, rows),
        check_vma=False,
    )
```

```python
import functools

import jax
import jax.numpy as jnp
from jax import lax
from jax.experimental import pallas as pl
from jax.experimental.pallas import tpu as pltpu
from jax.sharding import PartitionSpec as P

MESH = pl.DeviceIdType.MESH
NT = (((1,), (1,)), ((), ()))
TN = (((0,), (0,)), ((), ()))
F32, BF16 = jnp.float32, jnp.bfloat16
LIMIT = 41 * 2**20
LATE = 0
OWN, RIGHT, LEFT, OPP = range(4)
CHIP_STEP = (0, 1, 3, 2)

POS_A, POS_B, NEG_B, NEG_A, FWD_POS, FWD_NEG, SIB = range(7)
X0 = 10
SUM_SIB = 20
U2_POS, U2_NEG, U1_POS, U1_NEG, U3_POS, U3_NEG = range(24, 30)
N_COPIES = 30


def dot(a, b, dims):
    return lax.dot_general(a, b, dims, preferred_element_type=F32)


def kernel(n, x, dy, gate, up, wg_in, wu_in, wd_in,
           early, passed, wg, wu, sibst, accd, dyf, xf, dgs, dus, sibr, sumr,
           wd, accg, accu, act, gb, ub, dgb, dub, hb, sumst,
           send, recv, lsem, asem, ssem, wsem):
    rows, d = x.shape
    f = gate.shape[1]
    half = rows // 2
    me = lax.axis_index("tp")
    core = lax.rem(me, 2)
    chip = lax.div(me, 2)
    chips = n // 2
    right, left = lax.rem(me + 2, n), lax.rem(me + n - 2, n)
    sib = me + 1 - 2 * core

    def at(ref, start, size):
        if not isinstance(start, int):
            start = pl.multiple_of(start, size)
        return ref.at[pl.ds(start, size)]

    def slot(q, m, h=None):
        return (q * 2 + m) * rows + (0 if h is None else h * half)

    def token(q, m):
        ahead = CHIP_STEP[q] if isinstance(q, int) else q + lax.div(q, 2) * (5 - 2 * q)
        c = lax.rem(chip + ahead, chips)
        k = core + m - 2 * core * m
        return (c * 2 + k) * rows

    def remote(i, src, dst, to):
        return pltpu.make_async_remote_copy(
            src_ref=src, dst_ref=dst, send_sem=send.at[i], recv_sem=recv.at[i],
            device_id={"tp": to}, device_id_type=MESH)

    def gather_copies(base, own, full):
        blk = lambda q, m: at(full, slot(q, m), rows)
        hlf = lambda q, h: at(full, slot(q, 0, h), half)
        mine = lambda h: at(own, h * half, half)
        copies = {
            POS_A: (mine(0), hlf(LEFT, 0), right),
            POS_B: (mine(1), hlf(LEFT, 1), right),
            NEG_B: (mine(1), hlf(RIGHT, 1), left),
            NEG_A: (mine(0), hlf(RIGHT, 0), left),
            FWD_POS: (hlf(LEFT, 0), hlf(OPP, 0), right),
            FWD_NEG: (hlf(RIGHT, 1), hlf(OPP, 1), left),
            SIB + OWN: (own, blk(OWN, 1), sib),
        }
        for q in (RIGHT, LEFT, OPP):
            copies[SIB + q] = (blk(q, 0), blk(q, 1), sib)
        return {i: remote(base + i, *c) for i, c in copies.items()}

    cdy = gather_copies(0, dy, dyf)
    cx = gather_copies(X0, x, xf)
    stage = {OWN: 0, OPP: 1, RIGHT: 0, LEFT: 1}
    csib = [remote(SUM_SIB + q, sibst.at[stage[q]], at(sibr, q * rows, rows), sib) for q in range(4)]
    su = lambda i, s, to, dst: remote(i, sumst.at[s], dst, to)
    c2 = [su(U2_POS, 0, right, at(sumr, 0, half)), su(U2_NEG, 1, left, at(sumr, half, half))]
    c1 = [su(U1_POS, 2, right, at(sumr, 2 * half, half)), su(U1_NEG, 3, left, at(sumr, 3 * half, half))]
    c3 = [remote(i, passed.at[h], early.at[h], to) for i, h, to in ((U3_POS, 0, right), (U3_NEG, 1, left))]

    barrier = pltpu.get_barrier_semaphore()
    for other in (left, right, sib):
        pl.semaphore_signal(barrier, inc=1, device_id={"tp": other}, device_id_type=MESH)
    pl.semaphore_wait(barrier, 3)

    for i in (POS_A, NEG_B, POS_B, NEG_A, SIB + OWN):
        cdy[i].start()
    cx[SIB + OWN].start()
    weights = [pltpu.make_async_copy(s, t, wsem.at[i]) for i, (s, t) in enumerate(((wd_in, wd), (wg_in, wg), (wu_in, wu)))]
    weights[0].start()

    def load(src, dst, sem):
        return pltpu.make_async_copy(src, dst, sem)

    def start_block(own, full, first, second, q, m, r, b):
        big = act.at[b]
        if own is None:
            load(at(full, slot(q, m), rows), big, lsem.at[b, 0]).start()
        else:
            @pl.when(m == 0)
            def _():
                load(own, big, lsem.at[b, 0]).start()

            @pl.when(m != 0)
            def _():
                load(at(full, slot(q, m), rows), big, lsem.at[b, 0]).start()
        load(at(first, r, rows), gb.at[b], lsem.at[b, 1]).start()
        load(at(second, r, rows), ub.at[b], lsem.at[b, 2]).start()

    def wait_block(b):
        load(dy, act.at[b], lsem.at[b, 0]).wait()
        load(at(gate, 0, rows), gb.at[b], lsem.at[b, 1]).wait()
        load(at(gate, 0, rows), ub.at[b], lsem.at[b, 2]).wait()

    def blocks(count, place, ready, begin, compute):
        ready(0)
        begin(*place(0), 0)

        def body(i, _):
            b = lax.rem(i, 2)
            wait_block(b)

            @pl.when(i + 1 < count)
            def _():
                ready(i + 1)
                begin(*place(i + 1), 1 - b)

            compute(*place(i), b)
            return 0

        lax.fori_loop(0, count, body, 0)

    tile_f = 512 if f % 512 == 0 else f
    tile_d = 512 if d % 512 == 0 else d

    def begin_dy(own):
        return lambda q, m, b: start_block(own, dyf, gate, up, q, m, token(q, m), b)

    def from_dy(q, m, b):
        def columns(j, _):
            c = pl.ds(pl.multiple_of(j * tile_f, tile_f), tile_f)
            d_hidden = dot(act[b], wd[c, :], NT)
            g, u = gb[b, :, c].astype(F32), ub[b, :, c].astype(F32)
            s = lax.logistic(g)
            silu = g * s
            hb[:, c] = (silu * u).astype(BF16)
            dub[:, c] = (d_hidden * silu).astype(BF16)
            t = d_hidden * u
            dgb[:, c] = (t * s + t * g * (s * (1.0 - s))).astype(BF16)
            return 0

        lax.fori_loop(0, f // tile_f, columns, 0)
        r = slot(q, m)
        saves = [load(dgb, at(dgs, r, rows), ssem.at[0]), load(dub, at(dus, r, rows), ssem.at[1])]
        for s in saves:
            s.start()

        def hidden_columns(j, _):
            c = pl.ds(pl.multiple_of(j * tile_f, tile_f), tile_f)
            for k in range(0, d, d // 2):
                accd[c, k : k + d // 2] += dot(hb[:, c], act[b, :, k : k + d // 2], TN)
            return 0

        lax.fori_loop(0, f // tile_f, hidden_columns, 0)
        for s in saves:
            s.wait()

    def begin_x(own):
        return lambda q, m, b: start_block(own, xf, dgs, dus, q, m, slot(q, m), b)

    def from_x(q, m, b):
        def columns(j, _):
            c = pl.ds(pl.multiple_of(j * tile_d, tile_d), tile_d)
            xt = act[b, :, c]
            accg[c, :] += dot(xt, gb[b], TN)
            accu[c, :] += dot(xt, ub[b], TN)
            return 0

        lax.fori_loop(0, d // tile_d, columns, 0)

    def dx_jobs(*jobs):
        def loads(k):
            r, count, adds, *_ = jobs[k]
            b = k % 2
            copies = []
            if r is not None:
                copies.append(load(at(dgs, r, count), gb.at[b, pl.ds(0, count)], lsem.at[b, 1]))
                copies.append(load(at(dus, r, count), ub.at[b, pl.ds(0, count)], lsem.at[b, 2]))
            for i, a in enumerate(adds):
                copies.append(load(a, act.at[b, pl.ds(i * half, half)], asem.at[b, i]))
            return copies

        def begin(k):
            for c in jobs[k][3]:
                c.wait_recv()
            for c in loads(k):
                c.start()

        begin(0)
        for k, (r, count, adds, _, store, after) in enumerate(jobs):
            if k + 1 < len(jobs):
                begin(k + 1)
            for c in loads(k):
                c.wait()
            b = k % 2
            g, u = (gb.at[b], ub.at[b]) if r is not None else (dgb, dub)

            def columns(j, _, g=g, u=u, b=b, count=count, adds=adds, store=store):
                c = pl.ds(pl.multiple_of(j * tile_d, tile_d), tile_d)
                t = dot(g[:count, :], wg[c, :], NT) + dot(u[:count, :], wu[c, :], NT)
                for i in range(len(adds)):
                    t += act[b, i * half : (i + 1) * half, c].astype(F32)
                store(c, t)
                return 0

            lax.fori_loop(0, d // tile_d, columns, 0)
            after()

    def put(into):
        def store(c, t):
            into[:, c] = t.astype(BF16)

        return store

    def for_sibling(q, here=False, before=None, after=None):
        def done():
            csib[q].start()
            if before is not None:
                before.wait_send()
            if after is not None:
                after()

        return (None if here else slot(q, 1), rows, [], [], put(sibst.at[stage[q]]), done)

    def chip_sum(q, h, into, extra, ready, after):
        return (slot(q, 0, h), half, [at(sibr, q * rows + h * half, half), *extra], ready, put(into), after)

    def zero(ref):
        def body(i, _):
            ref[pl.ds(pl.multiple_of(i * 128, 128), 128), :] = jnp.zeros((128, ref.shape[1]), F32)
            return 0

        lax.fori_loop(0, ref.shape[0] // 128, body, 0)

    nothing = lambda i: None

    def ready_own(copies):
        def ready(i):
            if not isinstance(i, int):
                copies[SIB + OWN].wait_recv()

        return ready

    own_place = lambda i: (0, i)
    weights[1].start()
    weights[2].start()
    for ref in (accd, accg, accu):
        zero(ref)
    weights[0].wait()
    blocks(2, own_place, ready_own(cdy), begin_dy(dy), from_dy)
    weights[1].wait()
    weights[2].wait()
    dx_jobs(for_sibling(OWN, here=True))

    cdy[POS_A].wait_recv()
    cdy[NEG_B].wait_recv()
    cdy[FWD_POS].start()
    cdy[FWD_NEG].start()
    for i in (POS_A, NEG_B, POS_B, NEG_A):
        cx[i].start()
    blocks(2, own_place, ready_own(cx), begin_x(x), from_x)

    cdy[POS_B].wait_recv()
    cdy[NEG_A].wait_recv()
    cdy[SIB + RIGHT].start()
    cdy[SIB + LEFT].start()

    def ready_near(copies):
        def ready(i):
            if not isinstance(i, int):
                @pl.when(i == 2)
                def _():
                    copies[SIB + RIGHT].wait_recv()
                    copies[SIB + LEFT].wait_recv()

        return ready

    near_place = lambda i: (1 + lax.rem(i, 2), lax.div(i, 2)) if not isinstance(i, int) else (1 + i % 2, i // 2)
    blocks(4, near_place, ready_near(cdy), begin_dy(None), from_dy)
    cdy[FWD_POS].wait_recv()
    cdy[FWD_NEG].wait_recv()
    cdy[SIB + OPP].start()

    def ready_far(copies):
        def ready(i):
            if not isinstance(i, int):
                copies[SIB + OPP].wait_recv()

        return ready

    far_place = lambda i: (OPP, i)
    blocks(2, far_place, ready_far(cdy), begin_dy(None), from_dy)

    def forward_x():
        cx[POS_A].wait_recv()
        cx[NEG_B].wait_recv()
        cx[FWD_POS].start()
        cx[FWD_NEG].start()

    dx_jobs(
        for_sibling(OPP, here=True, before=csib[OWN]),
        for_sibling(RIGHT, before=csib[OPP], after=forward_x),
        for_sibling(LEFT),
        chip_sum(OPP, 0, sumst.at[2], [], [csib[OPP]], c1[0].start),
        chip_sum(OPP, 1, sumst.at[3], [], [], c1[1].start),
        chip_sum(RIGHT, 1, sumst.at[0], [], [csib[RIGHT]], c2[0].start),
        chip_sum(LEFT, 0, sumst.at[1], [], [csib[LEFT]], c2[1].start),
    )

    cx[POS_B].wait_recv()
    cx[NEG_A].wait_recv()
    cx[SIB + RIGHT].start()
    cx[SIB + LEFT].start()

    csib[RIGHT].wait_send()
    csib[LEFT].wait_send()
    for i in range(f // rows):
        sibst[i] = accd[i * rows : (i + 1) * rows, :].astype(BF16)

    blocks(4, near_place, ready_near(cx), begin_x(None), from_x)


    def hold(h):
        def store(c, t):
            accd[h * half : (h + 1) * half, c] = t

        ready = [csib[OWN]] if h == 0 else []
        return (slot(OWN, 0, h), half, [at(sibr, h * half, half)], ready, store, lambda: None)

    dx_jobs(hold(0), hold(1))

    cx[FWD_POS].wait_recv()
    cx[FWD_NEG].wait_recv()
    cx[SIB + OPP].start()
    blocks(2, far_place, ready_far(cx), begin_x(None), from_x)

    def passing(i, q, h):
        def after():
            @pl.when(core != LATE)
            def _():
                c3[i].start()

        return chip_sum(q, h, passed.at[i], [at(sumr, (2 + i) * half, half)], [c1[i]], after)

    dx_jobs(passing(0, RIGHT, 0), passing(1, LEFT, 1))

    for i in range(d // rows):
        r = slice(i * rows, (i + 1) * rows)
        wg[r, :] = accg[r, :].astype(BF16)
        wu[r, :] = accu[r, :].astype(BF16)
    for c in c2:
        c.wait_recv()
    for c in (*cdy.values(), *cx.values(), *c1, *c2):
        c.wait_send()

    @pl.when(core != LATE)
    def _():
        for c in c3:
            c.wait_recv()
            c.wait_send()


def write_weights(dwg_in, dwu_in, dwd_in, own, sumr, early, held, dwg, dwu, dwd, token, near, sem):
    core = lax.rem(lax.axis_index("tp"), 2)
    half = near.shape[1]
    rows = 2 * half
    adds = [pltpu.make_async_copy(sumr.at[pl.ds((1 - h) * half, half)], near.at[h], sem.at[h]) for h in range(2)]
    more = [pltpu.make_async_copy(early.at[h], near.at[2 + h], sem.at[2 + h]) for h in range(2)]
    copies = [pltpu.make_async_copy(s, t, sem.at[4 + i]) for i, (s, t) in enumerate(((dwg_in, dwg), (dwu_in, dwu)))]
    copies += [pltpu.make_async_copy(dwd_in.at[i], dwd.at[pl.ds(i * rows, rows)], sem.at[6 + i]) for i in range(dwd_in.shape[0])]
    for c in (*adds, *copies):
        c.start()
    token[...] = jnp.zeros_like(token)

    @pl.when(core != LATE)
    def _():
        for c in more:
            c.start()

    for h in range(2):
        adds[h].wait()
        r = slice(h * half, (h + 1) * half)
        held[r, :] = own[r, :] + near[h].astype(F32)

    @pl.when(core != LATE)
    def _():
        for h in range(2):
            more[h].wait()
            r = slice(h * half, (h + 1) * half)
            held[r, :] += near[2 + h].astype(F32)

    for c in copies:
        c.wait()


def pass_on(n, passed, held, token, dx, late, send, recv):
    me = lax.axis_index("tp")
    core = lax.rem(me, 2)
    right, left = lax.rem(me + 2, n), lax.rem(me + n - 2, n)
    half = passed.shape[1]
    barrier = pltpu.get_barrier_semaphore()
    for other in (left, right):
        pl.semaphore_signal(barrier, inc=1, device_id={"tp": other}, device_id_type=MESH)
    pl.semaphore_wait(barrier, 2)

    @pl.when(core == LATE)
    def _():
        copies = []
        for k, (start, count) in enumerate(((0, half - half // 16), (half - half // 16, half // 16))):
            for h, to in enumerate((right, left)):
                r = pl.ds(start, count)
                c = pltpu.make_async_remote_copy(
                    src_ref=passed.at[h, r], dst_ref=late.at[h, r], send_sem=send.at[h, k], recv_sem=recv.at[h, k],
                    device_id={"tp": to}, device_id_type=MESH)
                c.start()
                copies.append((c, h, start, count))
        for c, h, start, count in copies:
            c.wait_recv()
            r = slice(h * half + start, h * half + start + count)
            dx[r, :] = (held[r, :] + late[h, start : start + count, :].astype(F32)).astype(BF16)
        for c, *_ in copies:
            c.wait_send()

    @pl.when(core != LATE)
    def _():
        dx[...] = held[...].astype(BF16)


def finish(dx_in, dx, sem):
    parts = sem.shape[0]
    count = dx.shape[0] // parts
    copies = [pltpu.make_async_copy(dx_in.at[r], dx.at[r], sem.at[i]) for i in range(parts) for r in (pl.ds(i * count, count),)]
    for c in copies:
        c.start()
    for c in copies:
        c.wait()


def solution(mesh):
    n = mesh.shape["tp"]

    def local(x, dy, gate, up, wg, wu, wd):
        rows, d = x.shape
        tokens, f = gate.shape
        half = rows // 2
        hbm, vmem = pl.BlockSpec(memory_space=pltpu.HBM), pl.BlockSpec(memory_space=pltpu.VMEM)
        s = lambda *shape: jax.ShapeDtypeStruct(shape, BF16)
        v = lambda *shape: pltpu.VMEM(shape, BF16)
        a = lambda *shape: pltpu.VMEM(shape, F32)
        dma = pltpu.SemaphoreType.DMA
        flops = 12 * tokens * d * f
        early, passed, dwg, dwu, dwd, own, *_, sumr = pl.pallas_call(
            functools.partial(kernel, n),
            out_shape=(
                pltpu.HBM((2, half, d), BF16), v(2, half, d), v(d, f), v(d, f), v(f // rows, rows, d), a(f, d),
                s(tokens, d), s(tokens, d), s(tokens, f), s(tokens, f), s(4 * rows, d), pltpu.HBM((4 * half, d), BF16),
            ),
            in_specs=[hbm] * 7,
            out_specs=[hbm] + [vmem] * 5 + [hbm] * 6,
            scratch_shapes=[
                v(f, d), a(d, f), a(d, f),
                v(2, rows, d), v(2, rows, f), v(2, rows, f), v(rows, f), v(rows, f), v(rows, f), v(4, half, d),
                dma((N_COPIES,)), dma((N_COPIES,)), dma((2, 3)), dma((2, 2)), dma((2,)), dma((3,)),
            ],
            compiler_params=pltpu.CompilerParams(collective_id=0, has_side_effects=True, vmem_limit_bytes=LIMIT),
            cost_estimate=pl.CostEstimate(flops=flops, bytes_accessed=200 * 2**20, transcendentals=tokens * f),
            name="mlp_backward",
        )(x, dy, gate, up, wg, wu, wd)
        in_vmem = lambda t: pltpu.with_memory_space_constraint(t, pltpu.VMEM)
        small = pltpu.CompilerParams(vmem_limit_bytes=8 * 2**20)
        held, dwg, dwu, dwd, token = pl.pallas_call(
            write_weights,
            out_shape=(a(rows, d), s(d, f), s(d, f), s(f, d), v(8, 128)),
            in_specs=[vmem] * 4 + [hbm] * 2,
            out_specs=[vmem, hbm, hbm, hbm, vmem],
            scratch_shapes=[v(4, half, d), dma((6 + f // rows,))],
            compiler_params=small,
            name="write_weights",
        )(*map(in_vmem, (dwg, dwu, dwd, own)), *(pltpu.with_memory_space_constraint(t, pltpu.HBM) for t in (sumr, early)))
        dx = pl.pallas_call(
            functools.partial(pass_on, n),
            out_shape=v(rows, d),
            in_specs=[vmem] * 3,
            out_specs=vmem,
            scratch_shapes=[v(2, half, d), dma((2, 2)), dma((2, 2))],
            compiler_params=pltpu.CompilerParams(collective_id=1, has_side_effects=True, vmem_limit_bytes=8 * 2**20),
            name="pass_on",
        )(*map(in_vmem, (passed, held, token)))
        dx = pl.pallas_call(
            finish,
            out_shape=s(rows, d),
            in_specs=[vmem],
            out_specs=hbm,
            scratch_shapes=[dma((1,))],
            compiler_params=small,
            name="finish",
        )(in_vmem(dx))
        return dx, dwg, dwu, dwd

    rows, columns = P(("dp", "tp"), None), P("dp", "tp")
    return jax.shard_map(
        local,
        mesh=mesh,
        in_specs=(rows, rows, columns, columns, P(None, "tp"), P(None, "tp"), P("tp", None)),
        out_specs=(rows, columns, columns, rows),
        check_vma=False,
    )
```
